32 devices in a mesh: grid: 4 (over y, x), fsdp: 8 (over z, core).
Axes of the slice: x: 2, y: 2, z: 4, core: 2. Of those that a mesh axis runs over, the one named last changes fastest.
Arguments:
- hidden: bfloat16 [512, 4096], P('fsdp'), may hold values from -16 to 16
- norm_gain: float32 [4096], replicated, may hold values from 0.5 to 1.5
- base_head: bfloat16 [8192, 4096], P('fsdp'), may hold values from -1 to 1
- first_dir: bfloat16 [8192, 4096], P('fsdp'), may hold values from -0.09375 to 0.09375
- second_dir: bfloat16 [8192, 4096], P('fsdp'), may hold values from -0.09375 to 0.09375
- coords: int32 [8, 2], P('grid'), parts along dimension 0, may hold values from 0 to 7
- targets: int32 [512], replicated, may hold values from 0 to 8191
Outputs:
- token_loss: float32 [8, 512], P('grid', 'fsdp'), parts along dimension 0
- mean_loss: float32 [8], P('grid'), parts along dimension 0
The draws below stay inside these ranges and needn't reach their ends.
There are 4 independent parts, one for each index of `grid`. The reference program is written for one: setup_inputs(seed, part) draws one part's arguments, and reference() takes and returns one part's arrays. A program takes and returns all parts, laid end to end along the dimension named above; an argument that names none is the same for every part. Nothing has to cross between parts.
All inputs are finite; a program needn't handle non-finite values.
Results may differ from the reference program's by a relative error of at most 0.0003.
Values may be sent and summed in bfloat16 or wider, within the bound.
A program may use at most 128 MiB of HBM per device.

```python
import math
import jax
import jax.numpy as jnp
from jax import lax

D = 4096
V_DEV = 1024
PTS = 2
TOKENS = 512
VOCAB = 8192
N_FSDP = 8


def spike_plan(key):
    spike_key = jax.random.fold_in(key, 7177)
    spike_rows = jax.random.randint(jax.random.fold_in(spike_key, 1), (N_FSDP,), 0, TOKENS)
    offsets = jax.random.randint(jax.random.fold_in(spike_key, 2), (N_FSDP,), 0, V_DEV)
    spike_cols = jnp.arange(N_FSDP, dtype=jnp.int32) * V_DEV + offsets
    pattern = jnp.clip(jax.random.normal(jax.random.fold_in(spike_key, 3), (N_FSDP, D), jnp.float32), -3.0, 3.0)
    return (spike_rows, spike_cols, pattern)


def draw_hidden(key, part):
    rows_all = jnp.clip(jax.random.normal(jax.random.fold_in(key, 21), (TOKENS, D), jnp.float32), -4.0, 4.0)
    spike_rows, spike_cols, pattern = spike_plan(key)
    rows_all = rows_all.at[spike_rows].set(pattern)
    return rows_all.astype(jnp.bfloat16)


def draw_base_head(key, part):
    weight = jnp.clip(jax.random.normal(jax.random.fold_in(key, 11), (VOCAB, D), jnp.float32) / math.sqrt(D), -0.25, 0.25)
    spike_rows, spike_cols, pattern = spike_plan(key)
    weight = weight.at[spike_cols].set(240.0 / D * pattern)
    return weight.astype(jnp.bfloat16)


def touch_ends(result, key, low, high):
    longest = result.shape.index(max(result.shape))
    spots = []
    for shift in (0, 1):
        where = [jax.random.randint(jax.random.fold_in(key, axis), (), 0, length) for axis, length in enumerate(result.shape)]
        where[longest] = (where[longest] + shift) % result.shape[longest]
        spots.append(tuple(where))
    return result.at[spots[0]].set(low).at[spots[1]].set(high)


def block_levels(own_key, shape, pieces, low, top_value):
    loudness = 1.0
    for dim, blocks in pieces:
        draws = jax.random.uniform(jax.random.fold_in(jax.random.fold_in(own_key, 6), dim), (blocks,), jnp.float32, low / len(pieces), top_value / len(pieces))
        loudness = loudness * jnp.repeat(jnp.exp(draws), shape[dim] // blocks).reshape((-1,) + (1,) * (len(shape) - 1 - dim))
    return loudness


def bell_draw(own_key, extent, spread, bound, cuts=(), kind=jnp.bfloat16):
    entries = spread * jax.random.normal(own_key, extent, jnp.float32)
    if cuts:
        entries = entries * block_levels(own_key, extent, cuts, -0.22, 0.18)
    return jnp.clip(entries, -bound, bound).astype(kind)


def setup_inputs(seed: int = 0, part: int = 0) -> dict:
    keys = jax.random.split(jax.random.key(seed), 8)
    own_keys = jax.random.split(jax.random.fold_in(keys[7], part), 8)
    hidden = draw_hidden(jax.random.fold_in(keys[7], 71), part)
    norm_gain = jnp.clip(1.0 + 0.1 * jax.random.normal(keys[1], (D,), jnp.float32), 0.5, 1.5)
    base_head = draw_base_head(jax.random.fold_in(keys[7], 71), part)
    first_dir = bell_draw(keys[3], (VOCAB, D), D ** -0.5, 0.09375, ((0, 8),))
    second_dir = bell_draw(keys[4], (VOCAB, D), D ** -0.5, 0.09375, ((0, 8),))
    coords = touch_ends(jax.random.randint(own_keys[5], (PTS, 2), 0, 8), jax.random.fold_in(own_keys[5], 1), 0, 7).astype(jnp.int32)
    targets = touch_ends(jax.random.randint(keys[6], (TOKENS,), 0, VOCAB), jax.random.fold_in(keys[6], 1), 0, VOCAB - 1).astype(jnp.int32)
    return dict(hidden=hidden, norm_gain=norm_gain, base_head=base_head, first_dir=first_dir, second_dir=second_dir, coords=coords, targets=targets)


epsilon = 1e-05

def reference(hidden, norm_gain, base_head, first_dir, second_dir, coords, targets):
    level_table = (2.0 * jnp.arange(8, dtype=jnp.float32) - 7.0) / 7.0
    mixing = level_table[coords]
    widened = hidden.astype(jnp.float32)
    inv_rms = lax.rsqrt(lax.optimization_barrier(jnp.mean(widened * widened, axis=1, keepdims=True)) + epsilon)
    normed = (widened * inv_rms * norm_gain).astype(jnp.bfloat16)
    losses = []
    for point_idx in range(PTS):
        head_now = (base_head.astype(jnp.float32) + mixing[point_idx, 0] * first_dir.astype(jnp.float32) + mixing[point_idx, 1] * second_dir.astype(jnp.float32)).astype(jnp.bfloat16)
        logits = jnp.dot(normed, head_now.T, preferred_element_type=jnp.float32)
        row_top = lax.optimization_barrier(jnp.max(logits, axis=1, keepdims=True))
        log_total = row_top[:, 0] + jnp.log(lax.optimization_barrier(jnp.sum(jnp.exp(logits - row_top), axis=1)))
        picked = jnp.take_along_axis(logits, targets[:, None].astype(jnp.int32), axis=1)[:, 0]
        losses.append(log_total - picked)
    token_loss = jnp.stack(losses)
    return (token_loss, lax.optimization_barrier(jnp.mean(token_loss, axis=1)))
```

```python
import functools

import jax
import jax.numpy as jnp
from jax import lax
from jax.experimental import pallas as pl
from jax.experimental.pallas import tpu as pltpu
from jax.sharding import PartitionSpec as P

epsilon = 1e-05
MESH = pl.DeviceIdType.MESH
NUM_PIECES = 16
ROW_CHUNK = 32


def kernel(
    n_grid, n_fsdp, total_tokens,
    coords_ref, hidden_ref, gain_ref, targets_ref, base_ref, first_ref, second_ref,
    token_ref, mean_ref,
    w_buf, x_buf, acc, mix_own, mix_all, stat_own, stat_all,
    w_sem, up_sem, dn_sem, pt_sem, recv_sem, recv_pt_sem,
    mix_send, mix_recv, stat_send, stat_recv, known_sem,
):
    g = lax.axis_index("grid")
    f = lax.axis_index("fsdp")
    n_chips = n_fsdp // 2
    z, core = f // 2, f % 2
    n_all = n_grid * n_fsdp
    me = g * n_fsdp + f
    pts = coords_ref.shape[0]
    own, width = hidden_ref.shape
    vocab = base_ref.shape[0]
    kp = x_buf.shape[2]
    lanes = x_buf.shape[1]
    is_root = z == g
    go_up = jnp.logical_and(z >= g, z < n_chips - 1)
    go_dn = jnp.logical_and(z <= g, z > 0)

    def w_copy(j, p):
        src = (base_ref, first_ref, second_ref)[j]
        cols = pl.ds(pl.multiple_of(p * kp, kp), kp)
        return pltpu.make_async_copy(src.at[:, cols], w_buf.at[j, p], w_sem.at[j, p])

    barrier = pltpu.get_barrier_semaphore()
    for d in range(1, n_fsdp):
        pl.semaphore_signal(
            barrier, inc=1, device_id=(g, lax.rem(f + d, n_fsdp)), device_id_type=MESH
        )
    for d in range(1, n_grid):
        pl.semaphore_signal(
            barrier, inc=1, device_id=(lax.rem(g + d, n_grid), f), device_id_type=MESH
        )

    @pl.loop(0, NUM_PIECES)
    def _(p):
        for j in range(3):
            w_copy(j, p).start()

    for pt in range(pts):
        for k in range(2):
            level = jnp.full((1, lanes), coords_ref[pt, k], jnp.int32).astype(jnp.float32)
            mix_own[2 * pt + k : 2 * pt + k + 1, :] = (2.0 * level - 7.0) / 7.0
    mix_all[pl.ds(g, 1)] = mix_own[...][None]

    mine = pl.ds(pl.multiple_of(core * own, own), own)

    @pl.when(is_root)
    def _():
        squares = jnp.zeros((own, 1), jnp.float32)
        for p in range(NUM_PIECES):
            wide = hidden_ref[:, p * kp : (p + 1) * kp].astype(jnp.float32)
            squares = squares + jnp.sum(wide * wide, axis=1, keepdims=True)
        inv_rms = lax.rsqrt(squares / width + epsilon)
        for p in range(NUM_PIECES):
            wide = hidden_ref[:, p * kp : (p + 1) * kp].astype(jnp.float32)
            gain = gain_ref[:, p * kp : (p + 1) * kp]
            x_buf[p, mine, :] = (wide * inv_rms * gain).astype(jnp.bfloat16)

    pl.semaphore_wait(barrier, n_fsdp + n_grid - 2)

    def x_copy(p, send_sem, sem, target):
        return pltpu.make_async_remote_copy(
            src_ref=x_buf.at[p, mine], dst_ref=x_buf.at[p, mine],
            send_sem=send_sem.at[p], recv_sem=sem.at[p],
            device_id=(g, target), device_id_type=MESH,
        )

    partner = f + 1 - 2 * core
    above = lax.rem(f + 2, n_fsdp)
    below = lax.rem(f + n_fsdp - 2, n_fsdp)

    def send_on(p):
        @pl.when(go_up)
        def _():
            x_copy(p, up_sem, recv_sem, above).start()

        @pl.when(go_dn)
        def _():
            x_copy(p, dn_sem, recv_sem, below).start()

        x_copy(p, pt_sem, recv_pt_sem, partner).start()

    @pl.when(is_root)
    def _():
        @pl.loop(0, NUM_PIECES)
        def _(p):
            send_on(p)

    def mix_copy(d):
        to = lax.rem(g + d, n_grid)
        return pltpu.make_async_remote_copy(
            src_ref=mix_own, dst_ref=mix_all.at[g],
            send_sem=mix_send.at[d - 1], recv_sem=mix_recv.at[g],
            device_id=(to, f), device_id_type=MESH,
        )

    for d in range(1, n_grid):
        pl.semaphore_signal(
            known_sem, inc=1, device_id=(lax.rem(g + d, n_grid), f), device_id_type=MESH
        )
        mix_copy(d).start()

    acc[...] = jnp.zeros_like(acc)

    @pl.loop(0, NUM_PIECES)
    def _(p):
        @pl.when(jnp.logical_not(is_root))
        def _():
            x_copy(p, up_sem, recv_sem, above).wait_recv()
            send_on(p)

        other = pl.ds(pl.multiple_of((1 - core) * own, own), own)
        pltpu.make_async_remote_copy(
            src_ref=x_buf.at[p, other], dst_ref=x_buf.at[p, other],
            send_sem=pt_sem.at[p], recv_sem=recv_pt_sem.at[p],
            device_id=(g, partner), device_id_type=MESH,
        ).wait_recv()
        for j in range(3):
            w_copy(j, p).wait()
            acc[j] += lax.dot_general(
                w_buf[j, p], x_buf[p], (((1,), (1,)), ((), ())),
                preferred_element_type=jnp.float32,
            )

    for d in range(1, n_grid):
        pltpu.make_async_remote_copy(
            src_ref=mix_own, dst_ref=mix_all.at[lax.rem(g + d, n_grid)],
            send_sem=mix_send.at[d - 1], recv_sem=mix_recv.at[lax.rem(g + d, n_grid)],
            device_id=(lax.rem(g + d, n_grid), f), device_id_type=MESH,
        ).wait_recv()

    n_pts = n_grid * pts
    coef = []
    for pt in range(n_pts):
        rows = [mix_all[pt // pts, 2 * (pt % pts) + k : 2 * (pt % pts) + k + 1, :] for k in range(2)]
        coef.append([jnp.broadcast_to(r, (8, lanes)) for r in rows])

    targets = targets_ref[pl.ds(g, 1), :] - f * vocab
    steps = vocab // ROW_CHUNK
    tall = ROW_CHUNK // 8

    def block(c):
        rows = pl.ds(pl.multiple_of(c * ROW_CHUNK, ROW_CHUNK), ROW_CHUNK)
        return [acc[j, rows, :].reshape(tall, 8, lanes) for j in range(3)]

    def mixed(parts, pt):
        return parts[0] + coef[pt][0][None] * parts[1] + coef[pt][1][None] * parts[2]

    sub = lax.broadcasted_iota(jnp.int32, (tall, 8, lanes), 0) * 8 + lax.broadcasted_iota(
        jnp.int32, (tall, 8, lanes), 1
    )

    def top_step(c, carry):
        tops, picks = carry
        parts = block(c)
        hit = sub == (targets - c * ROW_CHUNK)[None]
        picks = tuple(
            pk + jnp.sum(jnp.where(hit, part, 0.0), axis=0) for pk, part in zip(picks, parts)
        )
        tops = tuple(
            jnp.maximum(tops[pt], jnp.max(mixed(parts, pt), axis=0)) for pt in range(n_pts)
        )
        return tops, picks

    low = jnp.full((8, lanes), -jnp.inf, jnp.float32)
    zero = jnp.zeros((8, lanes), jnp.float32)
    tops, picks = lax.fori_loop(0, steps, top_step, ((low,) * n_pts, (zero,) * 3))
    tops = [jnp.broadcast_to(jnp.max(t, axis=0, keepdims=True), (8, lanes)) for t in tops]
    picks = [jnp.sum(pk, axis=0, keepdims=True) for pk in picks]

    def sum_step(c, sums):
        parts = block(c)
        return tuple(
            sums[pt] + jnp.sum(jnp.exp(mixed(parts, pt) - tops[pt][None]), axis=0)
            for pt in range(n_pts)
        )

    sums = lax.fori_loop(0, steps, sum_step, (zero,) * n_pts)
    for pt in range(n_pts):
        at, row = pt // pts, pt % pts
        total = jnp.sum(sums[pt], axis=0, keepdims=True)
        stat_own[at, row : row + 1, :] = tops[pt][0:1] + jnp.log(total)
        stat_own[at, pts + row : pts + row + 1, :] = (
            picks[0] + coef[pt][0][0:1] * picks[1] + coef[pt][1][0:1] * picks[2]
        )
    stat_all[pl.ds(f, 1), pl.ds(g, 1)] = stat_own[pl.ds(g, 1)][None]

    @pl.loop(0, NUM_PIECES)
    def _(p):
        @pl.when(go_up)
        def _():
            x_copy(p, up_sem, recv_sem, above).wait_send()

        @pl.when(go_dn)
        def _():
            x_copy(p, dn_sem, recv_sem, below).wait_send()

        x_copy(p, pt_sem, recv_pt_sem, partner).wait_send()

    for d in range(1, n_grid):
        mix_copy(d).wait_send()
    pl.semaphore_wait(known_sem, n_grid - 1)

    def stat_copy(d):
        to = lax.rem(me + d, n_all)
        return pltpu.make_async_remote_copy(
            src_ref=stat_own.at[to // n_fsdp], dst_ref=stat_all.at[f, g],
            send_sem=stat_send.at[d - 1], recv_sem=stat_recv.at[me],
            device_id=(to // n_fsdp, lax.rem(to, n_fsdp)), device_id_type=MESH,
        )

    @pl.loop(1, n_all)
    def _(d):
        stat_copy(d).start()

    @pl.loop(1, n_all)
    def _(d):
        frm = lax.rem(me + d, n_all)
        fg, ff = frm // n_fsdp, lax.rem(frm, n_fsdp)
        pltpu.make_async_remote_copy(
            src_ref=stat_own.at[0], dst_ref=stat_all.at[ff, fg],
            send_sem=stat_send.at[d - 1], recv_sem=stat_recv.at[frm],
            device_id=(fg, ff), device_id_type=MESH,
        ).wait_recv()

    everything = jnp.zeros((pts, lanes), jnp.float32)
    chosen = jnp.zeros((pts, lanes), jnp.float32)
    for column in range(n_grid):
        here = stat_all[:, column]
        lse = here[:, :pts]
        top = jnp.max(lse, axis=0)
        loss = top + jnp.log(jnp.sum(jnp.exp(lse - top[None]), axis=0))
        loss = loss - jnp.sum(here[:, pts:], axis=0)
        everything = everything + loss
        chosen = jnp.where(z == column, loss, chosen)
    token_ref[...] = jnp.where(core == 0, chosen[:, :own], chosen[:, own:])
    for pt in range(pts):
        mean_ref[pt] = jnp.sum(everything[pt : pt + 1, :]) / total_tokens

    @pl.loop(1, n_all)
    def _(d):
        stat_copy(d).wait_send()


def body(n_grid, n_fsdp, hidden, norm_gain, base_head, first_dir, second_dir, coords, targets):
    own, width = hidden.shape
    vocab = base_head.shape[0]
    pts = coords.shape[0]
    total = targets.shape[0]
    lanes = total // n_grid
    assert lanes == 2 * own and n_fsdp == 2 * n_grid
    kp = width // NUM_PIECES
    n_all = n_grid * n_fsdp
    dma = pltpu.SemaphoreType.DMA
    vmem = pl.BlockSpec(memory_space=pltpu.VMEM)
    smem = pl.BlockSpec(memory_space=pltpu.SMEM)
    anywhere = pl.BlockSpec(memory_space=pl.ANY)
    token_loss, mean_loss = pl.pallas_call(
        functools.partial(kernel, n_grid, n_fsdp, total),
        out_shape=(
            jax.ShapeDtypeStruct((pts, own), jnp.float32),
            jax.ShapeDtypeStruct((pts,), jnp.float32),
        ),
        in_specs=[smem, vmem, vmem, vmem, anywhere, anywhere, anywhere],
        out_specs=(vmem, smem),
        scratch_shapes=[
            pltpu.VMEM((3, NUM_PIECES, vocab, kp), jnp.bfloat16),
            pltpu.VMEM((NUM_PIECES, lanes, kp), jnp.bfloat16),
            pltpu.VMEM((3, vocab, lanes), jnp.float32),
            pltpu.VMEM((2 * pts, lanes), jnp.float32),
            pltpu.VMEM((n_grid, 2 * pts, lanes), jnp.float32),
            pltpu.VMEM((n_grid, 2 * pts, lanes), jnp.float32),
            pltpu.VMEM((n_fsdp, n_grid, 2 * pts, lanes), jnp.float32),
            dma((3, NUM_PIECES)),
            dma((NUM_PIECES,)),
            dma((NUM_PIECES,)),
            dma((NUM_PIECES,)),
            dma((NUM_PIECES,)),
            dma((NUM_PIECES,)),
            dma((n_grid - 1,)),
            dma((n_grid,)),
            dma((n_all - 1,)),
            dma((n_all,)),
            pltpu.SemaphoreType.REGULAR,
        ],
        compiler_params=pltpu.CompilerParams(
            collective_id=0, has_side_effects=True, vmem_limit_bytes=60 * 1024 * 1024
        ),
    )(
        coords, hidden, norm_gain.reshape(1, width), targets.reshape(n_grid, lanes),
        base_head, first_dir, second_dir,
    )
    return (token_loss, mean_loss)


def solution(mesh):
    placed = (
        P("fsdp", None),
        P(),
        P("fsdp", None),
        P("fsdp", None),
        P("fsdp", None),
        P("grid", None),
        P(),
    )
    n_grid, n_fsdp = mesh.shape["grid"], mesh.shape["fsdp"]
    return jax.shard_map(
        functools.partial(body, n_grid, n_fsdp),
        mesh=mesh, in_specs=placed, out_specs=(P("grid", "fsdp"), P("grid")), check_vma=False,
    )
```

```python
import functools

import jax
import jax.numpy as jnp
from jax import lax
from jax.experimental import pallas as pl
from jax.experimental.pallas import tpu as pltpu
from jax.sharding import PartitionSpec as P

epsilon = 1e-05
MESH = pl.DeviceIdType.MESH
NUM_PIECES = 16
ROW_CHUNK = 32


def kernel(
    n_grid, n_fsdp, total_tokens,
    coords_ref, hidden_hbm, gain_ref, targets_ref, base_ref, first_ref, second_ref,
    token_ref, mean_ref,
    hidden_ref, hidden_sem, w_buf, x_buf, acc, mix_own, mix_all, stat_own, stat_all,
    w_sem, up_sem, dn_sem, pt_sem, recv_sem, recv_pt_sem,
    mix_send, mix_recv, stat_send, stat_recv, known_sem,
):
    g = lax.axis_index("grid")
    f = lax.axis_index("fsdp")
    n_chips = n_fsdp // 2
    z, core = f // 2, f % 2
    n_all = n_grid * n_fsdp
    me = g * n_fsdp + f
    pts = coords_ref.shape[0]
    own, width = hidden_hbm.shape
    vocab = base_ref.shape[0]
    kp = x_buf.shape[2]
    lanes = x_buf.shape[1]
    is_root = z == g
    go_up = jnp.logical_and(z >= g, z < n_chips - 1)
    go_dn = jnp.logical_and(z <= g, z > 0)

    def w_copy(j, p):
        src = (base_ref, first_ref, second_ref)[j]
        cols = pl.ds(pl.multiple_of(p * kp, kp), kp)
        return pltpu.make_async_copy(src.at[:, cols], w_buf.at[j, p], w_sem.at[j, p])

    barrier = pltpu.get_barrier_semaphore()
    for d in range(1, n_fsdp):
        pl.semaphore_signal(
            barrier, inc=1, device_id=(g, lax.rem(f + d, n_fsdp)), device_id_type=MESH
        )
    for d in range(1, n_grid):
        pl.semaphore_signal(
            barrier, inc=1, device_id=(lax.rem(g + d, n_grid), f), device_id_type=MESH
        )

    @pl.when(is_root)
    def _():
        pltpu.make_async_copy(hidden_hbm, hidden_ref, hidden_sem).start()

    @pl.loop(0, NUM_PIECES)
    def _(p):
        for j in range(3):
            w_copy(j, p).start()

    for pt in range(pts):
        for k in range(2):
            level = jnp.full((1, lanes), coords_ref[pt, k], jnp.int32).astype(jnp.float32)
            mix_own[2 * pt + k : 2 * pt + k + 1, :] = (2.0 * level - 7.0) / 7.0
    mix_all[pl.ds(g, 1)] = mix_own[...][None]

    mine = pl.ds(pl.multiple_of(core * own, own), own)

    @pl.when(is_root)
    def _():
        pltpu.make_async_copy(hidden_hbm, hidden_ref, hidden_sem).wait()
        squares = jnp.zeros((own, 1), jnp.float32)
        for p in range(NUM_PIECES):
            wide = hidden_ref[:, p * kp : (p + 1) * kp].astype(jnp.float32)
            squares = squares + jnp.sum(wide * wide, axis=1, keepdims=True)
        inv_rms = lax.rsqrt(squares / width + epsilon)
        for p in range(NUM_PIECES):
            wide = hidden_ref[:, p * kp : (p + 1) * kp].astype(jnp.float32)
            gain = gain_ref[:, p * kp : (p + 1) * kp]
            x_buf[p, mine, :] = (wide * inv_rms * gain).astype(jnp.bfloat16)

    pl.semaphore_wait(barrier, n_fsdp + n_grid - 2)

    def x_copy(p, send_sem, sem, target):
        return pltpu.make_async_remote_copy(
            src_ref=x_buf.at[p, mine], dst_ref=x_buf.at[p, mine],
            send_sem=send_sem.at[p], recv_sem=sem.at[p],
            device_id=(g, target), device_id_type=MESH,
        )

    partner = f + 1 - 2 * core
    above = lax.rem(f + 2, n_fsdp)
    below = lax.rem(f + n_fsdp - 2, n_fsdp)

    def send_on(p):
        @pl.when(go_up)
        def _():
            x_copy(p, up_sem, recv_sem, above).start()

        @pl.when(go_dn)
        def _():
            x_copy(p, dn_sem, recv_sem, below).start()

        x_copy(p, pt_sem, recv_pt_sem, partner).start()

    @pl.when(is_root)
    def _():
        @pl.loop(0, NUM_PIECES)
        def _(p):
            send_on(p)

    def mix_copy(d):
        to = lax.rem(g + d, n_grid)
        return pltpu.make_async_remote_copy(
            src_ref=mix_own, dst_ref=mix_all.at[g],
            send_sem=mix_send.at[d - 1], recv_sem=mix_recv.at[g],
            device_id=(to, f), device_id_type=MESH,
        )

    for d in range(1, n_grid):
        pl.semaphore_signal(
            known_sem, inc=1, device_id=(lax.rem(g + d, n_grid), f), device_id_type=MESH
        )
        mix_copy(d).start()

    acc[...] = jnp.zeros_like(acc)

    def compute(p):
        other = pl.ds(pl.multiple_of((1 - core) * own, own), own)
        pltpu.make_async_remote_copy(
            src_ref=x_buf.at[p, other], dst_ref=x_buf.at[p, other],
            send_sem=pt_sem.at[p], recv_sem=recv_pt_sem.at[p],
            device_id=(g, partner), device_id_type=MESH,
        ).wait_recv()
        for j in range(3):
            w_copy(j, p).wait()
            acc[j] += lax.dot_general(
                w_buf[j, p], x_buf[p], (((1,), (1,)), ((), ())),
                preferred_element_type=jnp.float32,
            )

    @pl.loop(0, NUM_PIECES)
    def _(p):
        @pl.when(jnp.logical_not(is_root))
        def _():
            x_copy(p, up_sem, recv_sem, above).wait_recv()
            send_on(p)

        @pl.when(p > 0)
        def _():
            compute(p - 1)

    compute(NUM_PIECES - 1)

    for d in range(1, n_grid):
        pltpu.make_async_remote_copy(
            src_ref=mix_own, dst_ref=mix_all.at[lax.rem(g + d, n_grid)],
            send_sem=mix_send.at[d - 1], recv_sem=mix_recv.at[lax.rem(g + d, n_grid)],
            device_id=(lax.rem(g + d, n_grid), f), device_id_type=MESH,
        ).wait_recv()

    n_pts = n_grid * pts
    coef = []
    for pt in range(n_pts):
        rows = [mix_all[pt // pts, 2 * (pt % pts) + k : 2 * (pt % pts) + k + 1, :] for k in range(2)]
        coef.append([jnp.broadcast_to(r, (8, lanes)) for r in rows])

    targets = targets_ref[pl.ds(g, 1), :] - f * vocab
    steps = vocab // ROW_CHUNK
    tall = ROW_CHUNK // 8

    def block(c):
        rows = pl.ds(pl.multiple_of(c * ROW_CHUNK, ROW_CHUNK), ROW_CHUNK)
        return [acc[j, rows, :].reshape(tall, 8, lanes) for j in range(3)]

    def mixed(parts, pt):
        return parts[0] + coef[pt][0][None] * parts[1] + coef[pt][1][None] * parts[2]

    sub = lax.broadcasted_iota(jnp.int32, (tall, 8, lanes), 0) * 8 + lax.broadcasted_iota(
        jnp.int32, (tall, 8, lanes), 1
    )

    def top_step(c, carry):
        tops, picks = carry
        parts = block(c)
        hit = sub == (targets - c * ROW_CHUNK)[None]
        picks = tuple(
            pk + jnp.sum(jnp.where(hit, part, 0.0), axis=0) for pk, part in zip(picks, parts)
        )
        tops = tuple(
            jnp.maximum(tops[pt], jnp.max(mixed(parts, pt), axis=0)) for pt in range(n_pts)
        )
        return tops, picks

    low = jnp.full((8, lanes), -jnp.inf, jnp.float32)
    zero = jnp.zeros((8, lanes), jnp.float32)
    tops, picks = lax.fori_loop(0, steps, top_step, ((low,) * n_pts, (zero,) * 3))
    tops = [jnp.broadcast_to(jnp.max(t, axis=0, keepdims=True), (8, lanes)) for t in tops]
    picks = [jnp.sum(pk, axis=0, keepdims=True) for pk in picks]

    def sum_step(c, sums):
        parts = block(c)
        return tuple(
            sums[pt] + jnp.sum(jnp.exp(mixed(parts, pt) - tops[pt][None]), axis=0)
            for pt in range(n_pts)
        )

    sums = lax.fori_loop(0, steps, sum_step, (zero,) * n_pts)
    for pt in range(n_pts):
        at, row = pt // pts, pt % pts
        total = jnp.sum(sums[pt], axis=0, keepdims=True)
        stat_own[at, row : row + 1, :] = tops[pt][0:1] + jnp.log(total)
        stat_own[at, pts + row : pts + row + 1, :] = (
            picks[0] + coef[pt][0][0:1] * picks[1] + coef[pt][1][0:1] * picks[2]
        )
    stat_all[pl.ds(f, 1), pl.ds(g, 1)] = stat_own[pl.ds(g, 1)][None]

    @pl.loop(0, NUM_PIECES)
    def _(p):
        @pl.when(go_up)
        def _():
            x_copy(p, up_sem, recv_sem, above).wait_send()

        @pl.when(go_dn)
        def _():
            x_copy(p, dn_sem, recv_sem, below).wait_send()

        x_copy(p, pt_sem, recv_pt_sem, partner).wait_send()

    for d in range(1, n_grid):
        mix_copy(d).wait_send()
    pl.semaphore_wait(known_sem, n_grid - 1)

    def stat_copy(d):
        to = lax.rem(me + d, n_all)
        return pltpu.make_async_remote_copy(
            src_ref=stat_own.at[to // n_fsdp], dst_ref=stat_all.at[f, g],
            send_sem=stat_send.at[d - 1], recv_sem=stat_recv.at[me],
            device_id=(to // n_fsdp, lax.rem(to, n_fsdp)), device_id_type=MESH,
        )

    @pl.loop(1, n_all)
    def _(d):
        stat_copy(d).start()

    @pl.loop(1, n_all)
    def _(d):
        frm = lax.rem(me + d, n_all)
        fg, ff = frm // n_fsdp, lax.rem(frm, n_fsdp)
        pltpu.make_async_remote_copy(
            src_ref=stat_own.at[0], dst_ref=stat_all.at[ff, fg],
            send_sem=stat_send.at[d - 1], recv_sem=stat_recv.at[frm],
            device_id=(fg, ff), device_id_type=MESH,
        ).wait_recv()

    everything = jnp.zeros((pts, lanes), jnp.float32)
    chosen = jnp.zeros((pts, lanes), jnp.float32)
    for column in range(n_grid):
        here = stat_all[:, column]
        lse = here[:, :pts]
        top = jnp.max(lse, axis=0)
        loss = top + jnp.log(jnp.sum(jnp.exp(lse - top[None]), axis=0))
        loss = loss - jnp.sum(here[:, pts:], axis=0)
        everything = everything + loss
        chosen = jnp.where(z == column, loss, chosen)
    token_ref[...] = jnp.where(core == 0, chosen[:, :own], chosen[:, own:])
    for pt in range(pts):
        mean_ref[pt] = jnp.sum(everything[pt : pt + 1, :]) / total_tokens

    @pl.loop(1, n_all)
    def _(d):
        stat_copy(d).wait_send()


def body(n_grid, n_fsdp, hidden, norm_gain, base_head, first_dir, second_dir, coords, targets):
    own, width = hidden.shape
    vocab = base_head.shape[0]
    pts = coords.shape[0]
    total = targets.shape[0]
    lanes = total // n_grid
    assert lanes == 2 * own and n_fsdp == 2 * n_grid
    kp = width // NUM_PIECES
    n_all = n_grid * n_fsdp
    dma = pltpu.SemaphoreType.DMA
    vmem = pl.BlockSpec(memory_space=pltpu.VMEM)
    smem = pl.BlockSpec(memory_space=pltpu.SMEM)
    anywhere = pl.BlockSpec(memory_space=pl.ANY)
    token_loss, mean_loss = pl.pallas_call(
        functools.partial(kernel, n_grid, n_fsdp, total),
        out_shape=(
            jax.ShapeDtypeStruct((pts, own), jnp.float32),
            jax.ShapeDtypeStruct((pts,), jnp.float32),
        ),
        in_specs=[smem, anywhere, vmem, vmem, anywhere, anywhere, anywhere],
        out_specs=(vmem, smem),
        scratch_shapes=[
            pltpu.VMEM((own, width), jnp.bfloat16),
            dma,
            pltpu.VMEM((3, NUM_PIECES, vocab, kp), jnp.bfloat16),
            pltpu.VMEM((NUM_PIECES, lanes, kp), jnp.bfloat16),
            pltpu.VMEM((3, vocab, lanes), jnp.float32),
            pltpu.VMEM((2 * pts, lanes), jnp.float32),
            pltpu.VMEM((n_grid, 2 * pts, lanes), jnp.float32),
            pltpu.VMEM((n_grid, 2 * pts, lanes), jnp.float32),
            pltpu.VMEM((n_fsdp, n_grid, 2 * pts, lanes), jnp.float32),
            dma((3, NUM_PIECES)),
            dma((NUM_PIECES,)),
            dma((NUM_PIECES,)),
            dma((NUM_PIECES,)),
            dma((NUM_PIECES,)),
            dma((NUM_PIECES,)),
            dma((n_grid - 1,)),
            dma((n_grid,)),
            dma((n_all - 1,)),
            dma((n_all,)),
            pltpu.SemaphoreType.REGULAR,
        ],
        compiler_params=pltpu.CompilerParams(
            collective_id=0, has_side_effects=True, vmem_limit_bytes=60 * 1024 * 1024
        ),
    )(
        coords, hidden, norm_gain.reshape(1, width), targets.reshape(n_grid, lanes),
        base_head, first_dir, second_dir,
    )
    return (token_loss, mean_loss)


def solution(mesh):
    placed = (
        P("fsdp", None),
        P(),
        P("fsdp", None),
        P("fsdp", None),
        P("fsdp", None),
        P("grid", None),
        P(),
    )
    n_grid, n_fsdp = mesh.shape["grid"], mesh.shape["fsdp"]
    return jax.shard_map(
        functools.partial(body, n_grid, n_fsdp),
        mesh=mesh, in_specs=placed, out_specs=(P("grid", "fsdp"), P("grid")), check_vma=False,
    )
```

```python
import functools

import jax
import jax.numpy as jnp
from jax import lax
from jax.experimental import pallas as pl
from jax.experimental.pallas import tpu as pltpu
from jax.sharding import PartitionSpec as P

epsilon = 1e-05
MESH = pl.DeviceIdType.MESH
NUM_PIECES = 16
ROW_CHUNK = 32


def kernel(
    n_grid, n_fsdp, total_tokens,
    coords_ref, hidden_hbm, gain_ref, targets_ref, base_ref, first_ref, second_ref,
    packed_ref,
    hidden_ref, hidden_sem, w_buf, x_buf, acc, mix_own, mix_all, stat_own, stat_all,
    w_sem, up_sem, dn_sem, pt_sem, recv_sem, recv_pt_sem,
    mix_send, mix_recv, stat_send, stat_recv, known_sem,
):
    g = lax.axis_index("grid")
    f = lax.axis_index("fsdp")
    n_chips = n_fsdp // 2
    z, core = f // 2, f % 2
    n_all = n_grid * n_fsdp
    me = g * n_fsdp + f
    pts = coords_ref.shape[0]
    own, width = hidden_hbm.shape
    vocab = base_ref.shape[0]
    kp = x_buf.shape[2]
    lanes = x_buf.shape[1]
    is_root = z == g
    go_up = jnp.logical_and(z >= g, z < n_chips - 1)
    go_dn = jnp.logical_and(z <= g, z > 0)

    def w_copy(j, p):
        src = (base_ref, first_ref, second_ref)[j]
        cols = pl.ds(pl.multiple_of(p * kp, kp), kp)
        return pltpu.make_async_copy(src.at[:, cols], w_buf.at[j, p], w_sem.at[j, p])

    barrier = pltpu.get_barrier_semaphore()
    for d in range(1, n_fsdp):
        pl.semaphore_signal(
            barrier, inc=1, device_id=(g, lax.rem(f + d, n_fsdp)), device_id_type=MESH
        )
    for d in range(1, n_grid):
        pl.semaphore_signal(
            barrier, inc=1, device_id=(lax.rem(g + d, n_grid), f), device_id_type=MESH
        )

    @pl.when(is_root)
    def _():
        pltpu.make_async_copy(hidden_hbm, hidden_ref, hidden_sem).start()


    for pt in range(pts):
        for k in range(2):
            level = jnp.full((1, lanes), coords_ref[pt, k], jnp.int32).astype(jnp.float32)
            mix_own[2 * pt + k : 2 * pt + k + 1, :] = (2.0 * level - 7.0) / 7.0
    mix_all[pl.ds(g, 1)] = mix_own[...][None]

    mine = pl.ds(pl.multiple_of(core * own, own), own)

    @pl.when(is_root)
    def _():
        pltpu.make_async_copy(hidden_hbm, hidden_ref, hidden_sem).wait()
        squares = jnp.zeros((own, 1), jnp.float32)
        for p in range(NUM_PIECES):
            wide = hidden_ref[:, p * kp : (p + 1) * kp].astype(jnp.float32)
            squares = squares + jnp.sum(wide * wide, axis=1, keepdims=True)
        inv_rms = lax.rsqrt(squares / width + epsilon)
        for p in range(NUM_PIECES):
            wide = hidden_ref[:, p * kp : (p + 1) * kp].astype(jnp.float32)
            gain = gain_ref[:, p * kp : (p + 1) * kp]
            x_buf[p, mine, :] = (wide * inv_rms * gain).astype(jnp.bfloat16)

    pl.semaphore_wait(barrier, n_fsdp + n_grid - 2)

    def x_copy(p, send_sem, sem, target):
        return pltpu.make_async_remote_copy(
            src_ref=x_buf.at[p, mine], dst_ref=x_buf.at[p, mine],
            send_sem=send_sem.at[p], recv_sem=sem.at[p],
            device_id=(g, target), device_id_type=MESH,
        )

    partner = f + 1 - 2 * core
    above = lax.rem(f + 2, n_fsdp)
    below = lax.rem(f + n_fsdp - 2, n_fsdp)

    def send_on(p):
        @pl.when(go_up)
        def _():
            x_copy(p, up_sem, recv_sem, above).start()

        @pl.when(go_dn)
        def _():
            x_copy(p, dn_sem, recv_sem, below).start()

        x_copy(p, pt_sem, recv_pt_sem, partner).start()

    @pl.when(is_root)
    def _():
        @pl.loop(0, NUM_PIECES)
        def _(p):
            send_on(p)

    def mix_copy(d):
        to = lax.rem(g + d, n_grid)
        return pltpu.make_async_remote_copy(
            src_ref=mix_own, dst_ref=mix_all.at[g],
            send_sem=mix_send.at[d - 1], recv_sem=mix_recv.at[g],
            device_id=(to, f), device_id_type=MESH,
        )

    for d in range(1, n_grid):
        pl.semaphore_signal(
            known_sem, inc=1, device_id=(lax.rem(g + d, n_grid), f), device_id_type=MESH
        )
        mix_copy(d).start()

    @pl.loop(0, NUM_PIECES)
    def _(p):
        for j in range(3):
            w_copy(j, p).start()

    acc[...] = jnp.zeros_like(acc)

    def compute(p):
        other = pl.ds(pl.multiple_of((1 - core) * own, own), own)
        pltpu.make_async_remote_copy(
            src_ref=x_buf.at[p, other], dst_ref=x_buf.at[p, other],
            send_sem=pt_sem.at[p], recv_sem=recv_pt_sem.at[p],
            device_id=(g, partner), device_id_type=MESH,
        ).wait_recv()
        for j in range(3):
            w_copy(j, p).wait()
        for j in range(3):
            acc[j] += lax.dot_general(
                w_buf[j, p], x_buf[p], (((1,), (1,)), ((), ())),
                preferred_element_type=jnp.float32,
            )

    @pl.loop(0, NUM_PIECES)
    def _(p):
        @pl.when(jnp.logical_not(is_root))
        def _():
            x_copy(p, up_sem, recv_sem, above).wait_recv()
            send_on(p)

        @pl.when(p > 0)
        def _():
            compute(p - 1)

    compute(NUM_PIECES - 1)

    for d in range(1, n_grid):
        pltpu.make_async_remote_copy(
            src_ref=mix_own, dst_ref=mix_all.at[lax.rem(g + d, n_grid)],
            send_sem=mix_send.at[d - 1], recv_sem=mix_recv.at[lax.rem(g + d, n_grid)],
            device_id=(lax.rem(g + d, n_grid), f), device_id_type=MESH,
        ).wait_recv()

    n_pts = n_grid * pts
    coef = []
    for pt in range(n_pts):
        rows = [mix_all[pt // pts, 2 * (pt % pts) + k : 2 * (pt % pts) + k + 1, :] for k in range(2)]
        coef.append([jnp.broadcast_to(r, (8, lanes)) for r in rows])

    targets = targets_ref[pl.ds(g, 1), :] - f * vocab
    steps = vocab // ROW_CHUNK
    tall = ROW_CHUNK // 8

    def block(c):
        rows = pl.ds(pl.multiple_of(c * ROW_CHUNK, ROW_CHUNK), ROW_CHUNK)
        return [acc[j, rows, :].reshape(tall, 8, lanes) for j in range(3)]

    def mixed(parts, pt):
        return parts[0] + coef[pt][0][None] * parts[1] + coef[pt][1][None] * parts[2]

    sub = lax.broadcasted_iota(jnp.int32, (tall, 8, lanes), 0) * 8 + lax.broadcasted_iota(
        jnp.int32, (tall, 8, lanes), 1
    )

    def top_step(c, carry):
        tops, picks = carry
        parts = block(c)
        hit = sub == (targets - c * ROW_CHUNK)[None]
        picks = tuple(
            pk + jnp.sum(jnp.where(hit, part, 0.0), axis=0) for pk, part in zip(picks, parts)
        )
        tops = tuple(
            jnp.maximum(tops[pt], jnp.max(mixed(parts, pt), axis=0)) for pt in range(n_pts)
        )
        return tops, picks

    low = jnp.full((8, lanes), -jnp.inf, jnp.float32)
    zero = jnp.zeros((8, lanes), jnp.float32)
    tops, picks = lax.fori_loop(0, steps, top_step, ((low,) * n_pts, (zero,) * 3))
    tops = [jnp.broadcast_to(jnp.max(t, axis=0, keepdims=True), (8, lanes)) for t in tops]
    picks = [jnp.sum(pk, axis=0, keepdims=True) for pk in picks]

    def sum_step(c, sums):
        parts = block(c)
        return tuple(
            sums[pt] + jnp.sum(jnp.exp(mixed(parts, pt) - tops[pt][None]), axis=0)
            for pt in range(n_pts)
        )

    sums = lax.fori_loop(0, steps, sum_step, (zero,) * n_pts)
    for pt in range(n_pts):
        at, row = pt // pts, pt % pts
        total = jnp.sum(sums[pt], axis=0, keepdims=True)
        stat_own[at, row : row + 1, :] = tops[pt][0:1] + jnp.log(total)
        stat_own[at, pts + row : pts + row + 1, :] = (
            picks[0] + coef[pt][0][0:1] * picks[1] + coef[pt][1][0:1] * picks[2]
        )
    stat_all[pl.ds(f, 1), pl.ds(g, 1)] = stat_own[pl.ds(g, 1)][None]

    @pl.loop(0, NUM_PIECES)
    def _(p):
        @pl.when(go_up)
        def _():
            x_copy(p, up_sem, recv_sem, above).wait_send()

        @pl.when(go_dn)
        def _():
            x_copy(p, dn_sem, recv_sem, below).wait_send()

        x_copy(p, pt_sem, recv_pt_sem, partner).wait_send()

    for d in range(1, n_grid):
        mix_copy(d).wait_send()
    pl.semaphore_wait(known_sem, n_grid - 1)

    def stat_copy(d):
        to = lax.rem(me + d, n_all)
        return pltpu.make_async_remote_copy(
            src_ref=stat_own.at[to // n_fsdp], dst_ref=stat_all.at[f, g],
            send_sem=stat_send.at[d - 1], recv_sem=stat_recv.at[me],
            device_id=(to // n_fsdp, lax.rem(to, n_fsdp)), device_id_type=MESH,
        )

    @pl.loop(1, n_all)
    def _(d):
        stat_copy(d).start()

    @pl.loop(1, n_all)
    def _(d):
        frm = lax.rem(me + d, n_all)
        fg, ff = frm // n_fsdp, lax.rem(frm, n_fsdp)
        pltpu.make_async_remote_copy(
            src_ref=stat_own.at[0], dst_ref=stat_all.at[ff, fg],
            send_sem=stat_send.at[d - 1], recv_sem=stat_recv.at[frm],
            device_id=(fg, ff), device_id_type=MESH,
        ).wait_recv()

    everything = jnp.zeros((pts, lanes), jnp.float32)
    chosen = jnp.zeros((pts, lanes), jnp.float32)
    for column in range(n_grid):
        here = stat_all[:, column]
        lse = here[:, :pts]
        top = jnp.max(lse, axis=0)
        loss = top + jnp.log(jnp.sum(jnp.exp(lse - top[None]), axis=0))
        loss = loss - jnp.sum(here[:, pts:], axis=0)
        everything = everything + loss
        chosen = jnp.where(z == column, loss, chosen)
    packed_ref[:pts, :own] = jnp.where(core == 0, chosen[:, :own], chosen[:, own:])
    for pt in range(pts):
        mean = jnp.sum(everything[pt : pt + 1, :], axis=1, keepdims=True) / total_tokens
        packed_ref[pts + pt : pts + pt + 1, :] = jnp.broadcast_to(mean, (1, lanes))

    @pl.loop(1, n_all)
    def _(d):
        stat_copy(d).wait_send()


def split(packed_ref, token_ref, mean_ref):
    pts, own = token_ref.shape
    token_ref[...] = packed_ref[:pts, :own]
    for pt in range(pts):
        mean_ref[pt] = packed_ref[pts + pt, 0]


def body(n_grid, n_fsdp, hidden, norm_gain, base_head, first_dir, second_dir, coords, targets):
    own, width = hidden.shape
    vocab = base_head.shape[0]
    pts = coords.shape[0]
    total = targets.shape[0]
    lanes = total // n_grid
    assert lanes == 2 * own and n_fsdp == 2 * n_grid
    kp = width // NUM_PIECES
    n_all = n_grid * n_fsdp
    dma = pltpu.SemaphoreType.DMA
    vmem = pl.BlockSpec(memory_space=pltpu.VMEM)
    smem = pl.BlockSpec(memory_space=pltpu.SMEM)
    anywhere = pl.BlockSpec(memory_space=pl.ANY)
    packed = pl.pallas_call(
        functools.partial(kernel, n_grid, n_fsdp, total),
        out_shape=jax.ShapeDtypeStruct((2 * pts, lanes), jnp.float32),
        in_specs=[smem, anywhere, vmem, vmem, anywhere, anywhere, anywhere],
        out_specs=vmem,
        scratch_shapes=[
            pltpu.VMEM((own, width), jnp.bfloat16),
            dma,
            pltpu.VMEM((3, NUM_PIECES, vocab, kp), jnp.bfloat16),
            pltpu.VMEM((NUM_PIECES, lanes, kp), jnp.bfloat16),
            pltpu.VMEM((3, vocab, lanes), jnp.float32),
            pltpu.VMEM((2 * pts, lanes), jnp.float32),
            pltpu.VMEM((n_grid, 2 * pts, lanes), jnp.float32),
            pltpu.VMEM((n_grid, 2 * pts, lanes), jnp.float32),
            pltpu.VMEM((n_fsdp, n_grid, 2 * pts, lanes), jnp.float32),
            dma((3, NUM_PIECES)),
            dma((NUM_PIECES,)),
            dma((NUM_PIECES,)),
            dma((NUM_PIECES,)),
            dma((NUM_PIECES,)),
            dma((NUM_PIECES,)),
            dma((n_grid - 1,)),
            dma((n_grid,)),
            dma((n_all - 1,)),
            dma((n_all,)),
            pltpu.SemaphoreType.REGULAR,
        ],
        compiler_params=pltpu.CompilerParams(
            collective_id=0, has_side_effects=True, vmem_limit_bytes=60 * 1024 * 1024
        ),
    )(
        coords, hidden, norm_gain.reshape(1, width), targets.reshape(n_grid, lanes),
        base_head, first_dir, second_dir,
    )
    return tuple(
        pl.pallas_call(
            split,
            out_shape=(
                jax.ShapeDtypeStruct((pts, own), jnp.float32),
                jax.ShapeDtypeStruct((pts,), jnp.float32),
            ),
            in_specs=[vmem],
            out_specs=(vmem, smem),
        )(packed)
    )


def solution(mesh):
    placed = (
        P("fsdp", None),
        P(),
        P("fsdp", None),
        P("fsdp", None),
        P("fsdp", None),
        P("grid", None),
        P(),
    )
    n_grid, n_fsdp = mesh.shape["grid"], mesh.shape["fsdp"]
    return jax.shard_map(
        functools.partial(body, n_grid, n_fsdp),
        mesh=mesh, in_specs=placed, out_specs=(P("grid", "fsdp"), P("grid")), check_vma=False,
    )
```

```python
import functools

import jax
import jax.numpy as jnp
from jax import lax
from jax.experimental import pallas as pl
from jax.experimental.pallas import tpu as pltpu
from jax.sharding import PartitionSpec as P

epsilon = 1e-05
MESH = pl.DeviceIdType.MESH
NUM_PIECES = 16
ROW_CHUNK = 64


def kernel(
    n_grid, n_fsdp, total_tokens,
    coords_ref, hidden_hbm, gain_ref, targets_ref, base_ref, first_ref, second_ref,
    packed_ref,
    hidden_ref, hidden_sem, w_buf, x_buf, acc, mix_own, mix_all, stat_own, stat_all,
    w_sem, up_sem, dn_sem, pt_sem, recv_sem, recv_pt_sem,
    mix_send, mix_recv, stat_send, stat_recv, known_sem,
):
    g = lax.axis_index("grid")
    f = lax.axis_index("fsdp")
    n_chips = n_fsdp // 2
    z, core = f // 2, f % 2
    n_all = n_grid * n_fsdp
    me = g * n_fsdp + f
    pts = coords_ref.shape[0]
    own, width = hidden_hbm.shape
    vocab = base_ref.shape[0]
    kp = x_buf.shape[2]
    lanes = x_buf.shape[1]
    is_root = z == g
    go_up = jnp.logical_and(z >= g, z < n_chips - 1)
    go_dn = jnp.logical_and(z <= g, z > 0)

    def w_copy(j, p):
        src = (base_ref, first_ref, second_ref)[j]
        cols = pl.ds(pl.multiple_of(p * kp, kp), kp)
        return pltpu.make_async_copy(src.at[:, cols], w_buf.at[j, p], w_sem.at[j, p])

    barrier = pltpu.get_barrier_semaphore()
    for d in range(1, n_fsdp):
        pl.semaphore_signal(
            barrier, inc=1, device_id=(g, lax.rem(f + d, n_fsdp)), device_id_type=MESH
        )
    for d in range(1, n_grid):
        pl.semaphore_signal(
            barrier, inc=1, device_id=(lax.rem(g + d, n_grid), f), device_id_type=MESH
        )

    @pl.when(is_root)
    def _():
        pltpu.make_async_copy(hidden_hbm, hidden_ref, hidden_sem).start()


    for pt in range(pts):
        for k in range(2):
            level = jnp.full((1, lanes), coords_ref[pt, k], jnp.int32).astype(jnp.float32)
            mix_own[2 * pt + k : 2 * pt + k + 1, :] = (2.0 * level - 7.0) / 7.0
    mix_all[pl.ds(g, 1)] = mix_own[...][None]

    mine = pl.ds(pl.multiple_of(core * own, own), own)

    @pl.when(is_root)
    def _():
        pltpu.make_async_copy(hidden_hbm, hidden_ref, hidden_sem).wait()
        squares = jnp.zeros((own, 1), jnp.float32)
        for p in range(NUM_PIECES):
            wide = hidden_ref[:, p * kp : (p + 1) * kp].astype(jnp.float32)
            squares = squares + jnp.sum(wide * wide, axis=1, keepdims=True)
        inv_rms = lax.rsqrt(squares / width + epsilon)
        for p in range(NUM_PIECES):
            wide = hidden_ref[:, p * kp : (p + 1) * kp].astype(jnp.float32)
            gain = gain_ref[:, p * kp : (p + 1) * kp]
            x_buf[p, mine, :] = (wide * inv_rms * gain).astype(jnp.bfloat16)

    pl.semaphore_wait(barrier, n_fsdp + n_grid - 2)

    def x_copy(p, send_sem, sem, target):
        return pltpu.make_async_remote_copy(
            src_ref=x_buf.at[p, mine], dst_ref=x_buf.at[p, mine],
            send_sem=send_sem.at[p], recv_sem=sem.at[p],
            device_id=(g, target), device_id_type=MESH,
        )

    partner = f + 1 - 2 * core
    above = lax.rem(f + 2, n_fsdp)
    below = lax.rem(f + n_fsdp - 2, n_fsdp)

    def send_on(p):
        @pl.when(go_up)
        def _():
            x_copy(p, up_sem, recv_sem, above).start()

        @pl.when(go_dn)
        def _():
            x_copy(p, dn_sem, recv_sem, below).start()

        x_copy(p, pt_sem, recv_pt_sem, partner).start()

    @pl.when(is_root)
    def _():
        @pl.loop(0, NUM_PIECES)
        def _(p):
            send_on(p)

    def mix_copy(d):
        to = lax.rem(g + d, n_grid)
        return pltpu.make_async_remote_copy(
            src_ref=mix_own, dst_ref=mix_all.at[g],
            send_sem=mix_send.at[d - 1], recv_sem=mix_recv.at[g],
            device_id=(to, f), device_id_type=MESH,
        )

    for d in range(1, n_grid):
        pl.semaphore_signal(
            known_sem, inc=1, device_id=(lax.rem(g + d, n_grid), f), device_id_type=MESH
        )
        mix_copy(d).start()

    @pl.loop(0, NUM_PIECES)
    def _(p):
        for j in range(3):
            w_copy(j, p).start()

    acc[...] = jnp.zeros_like(acc)

    def compute(p):
        other = pl.ds(pl.multiple_of((1 - core) * own, own), own)
        pltpu.make_async_remote_copy(
            src_ref=x_buf.at[p, other], dst_ref=x_buf.at[p, other],
            send_sem=pt_sem.at[p], recv_sem=recv_pt_sem.at[p],
            device_id=(g, partner), device_id_type=MESH,
        ).wait_recv()
        for j in range(3):
            w_copy(j, p).wait()
        for j in range(3):
            acc[j] += lax.dot_general(
                w_buf[j, p], x_buf[p], (((1,), (1,)), ((), ())),
                preferred_element_type=jnp.float32,
            )

    @pl.loop(0, NUM_PIECES)
    def _(p):
        @pl.when(jnp.logical_not(is_root))
        def _():
            x_copy(p, up_sem, recv_sem, above).wait_recv()
            send_on(p)

        @pl.when(p > 0)
        def _():
            compute(p - 1)

    compute(NUM_PIECES - 1)

    for d in range(1, n_grid):
        pltpu.make_async_remote_copy(
            src_ref=mix_own, dst_ref=mix_all.at[lax.rem(g + d, n_grid)],
            send_sem=mix_send.at[d - 1], recv_sem=mix_recv.at[lax.rem(g + d, n_grid)],
            device_id=(lax.rem(g + d, n_grid), f), device_id_type=MESH,
        ).wait_recv()

    n_pts = n_grid * pts
    coef = []
    for pt in range(n_pts):
        rows = [mix_all[pt // pts, 2 * (pt % pts) + k : 2 * (pt % pts) + k + 1, :] for k in range(2)]
        coef.append([jnp.broadcast_to(r, (8, lanes)) for r in rows])

    targets = targets_ref[pl.ds(g, 1), :] - f * vocab
    steps = vocab // ROW_CHUNK
    tall = ROW_CHUNK // 8

    def block(c):
        rows = pl.ds(pl.multiple_of(c * ROW_CHUNK, ROW_CHUNK), ROW_CHUNK)
        return [acc[j, rows, :].reshape(tall, 8, lanes) for j in range(3)]

    def mixed(parts, pt):
        return parts[0] + coef[pt][0][None] * parts[1] + coef[pt][1][None] * parts[2]

    sub = lax.broadcasted_iota(jnp.int32, (tall, 8, lanes), 0) * 8 + lax.broadcasted_iota(
        jnp.int32, (tall, 8, lanes), 1
    )

    def top_step(c, carry):
        tops, picks = carry
        parts = block(c)
        hit = sub == (targets - c * ROW_CHUNK)[None]
        picks = tuple(
            pk + jnp.sum(jnp.where(hit, part, 0.0), axis=0) for pk, part in zip(picks, parts)
        )
        tops = tuple(
            jnp.maximum(tops[pt], jnp.max(mixed(parts, pt), axis=0)) for pt in range(n_pts)
        )
        return tops, picks

    low = jnp.full((8, lanes), -jnp.inf, jnp.float32)
    zero = jnp.zeros((8, lanes), jnp.float32)
    tops, picks = lax.fori_loop(0, steps, top_step, ((low,) * n_pts, (zero,) * 3))
    tops = [jnp.broadcast_to(jnp.max(t, axis=0, keepdims=True), (8, lanes)) for t in tops]
    picks = [jnp.sum(pk, axis=0, keepdims=True) for pk in picks]

    def sum_step(c, sums):
        parts = block(c)
        return tuple(
            sums[pt] + jnp.sum(jnp.exp(mixed(parts, pt) - tops[pt][None]), axis=0)
            for pt in range(n_pts)
        )

    sums = lax.fori_loop(0, steps, sum_step, (zero,) * n_pts)
    for pt in range(n_pts):
        at, row = pt // pts, pt % pts
        total = jnp.sum(sums[pt], axis=0, keepdims=True)
        stat_own[at, row : row + 1, :] = tops[pt][0:1] + jnp.log(total)
        stat_own[at, pts + row : pts + row + 1, :] = (
            picks[0] + coef[pt][0][0:1] * picks[1] + coef[pt][1][0:1] * picks[2]
        )
    stat_all[pl.ds(f, 1), pl.ds(g, 1)] = stat_own[pl.ds(g, 1)][None]

    @pl.loop(0, NUM_PIECES)
    def _(p):
        @pl.when(go_up)
        def _():
            x_copy(p, up_sem, recv_sem, above).wait_send()

        @pl.when(go_dn)
        def _():
            x_copy(p, dn_sem, recv_sem, below).wait_send()

        x_copy(p, pt_sem, recv_pt_sem, partner).wait_send()

    for d in range(1, n_grid):
        mix_copy(d).wait_send()
    pl.semaphore_wait(known_sem, n_grid - 1)

    def stat_copy(d):
        to = lax.rem(me + d, n_all)
        return pltpu.make_async_remote_copy(
            src_ref=stat_own.at[to // n_fsdp], dst_ref=stat_all.at[f, g],
            send_sem=stat_send.at[d - 1], recv_sem=stat_recv.at[me],
            device_id=(to // n_fsdp, lax.rem(to, n_fsdp)), device_id_type=MESH,
        )

    @pl.loop(1, n_all)
    def _(d):
        stat_copy(d).start()

    @pl.loop(1, n_all)
    def _(d):
        frm = lax.rem(me + d, n_all)
        fg, ff = frm // n_fsdp, lax.rem(frm, n_fsdp)
        pltpu.make_async_remote_copy(
            src_ref=stat_own.at[0], dst_ref=stat_all.at[ff, fg],
            send_sem=stat_send.at[d - 1], recv_sem=stat_recv.at[frm],
            device_id=(fg, ff), device_id_type=MESH,
        ).wait_recv()

    everything = jnp.zeros((pts, lanes), jnp.float32)
    chosen = jnp.zeros((pts, lanes), jnp.float32)
    for column in range(n_grid):
        here = stat_all[:, column]
        lse = here[:, :pts]
        top = jnp.max(lse, axis=0)
        loss = top + jnp.log(jnp.sum(jnp.exp(lse - top[None]), axis=0))
        loss = loss - jnp.sum(here[:, pts:], axis=0)
        everything = everything + loss
        chosen = jnp.where(z == column, loss, chosen)
    packed_ref[:pts, :own] = jnp.where(core == 0, chosen[:, :own], chosen[:, own:])
    for pt in range(pts):
        mean = jnp.sum(everything[pt : pt + 1, :], axis=1, keepdims=True) / total_tokens
        packed_ref[pts + pt : pts + pt + 1, :] = jnp.broadcast_to(mean, (1, lanes))

    @pl.loop(1, n_all)
    def _(d):
        stat_copy(d).wait_send()


def split(packed_ref, token_ref, mean_ref):
    pts, own = token_ref.shape
    token_ref[...] = packed_ref[:pts, :own]
    for pt in range(pts):
        mean_ref[pt] = packed_ref[pts + pt, 0]


def body(n_grid, n_fsdp, hidden, norm_gain, base_head, first_dir, second_dir, coords, targets):
    own, width = hidden.shape
    vocab = base_head.shape[0]
    pts = coords.shape[0]
    total = targets.shape[0]
    lanes = total // n_grid
    assert lanes == 2 * own and n_fsdp == 2 * n_grid
    kp = width // NUM_PIECES
    n_all = n_grid * n_fsdp
    dma = pltpu.SemaphoreType.DMA
    vmem = pl.BlockSpec(memory_space=pltpu.VMEM)
    smem = pl.BlockSpec(memory_space=pltpu.SMEM)
    anywhere = pl.BlockSpec(memory_space=pl.ANY)
    packed = pl.pallas_call(
        functools.partial(kernel, n_grid, n_fsdp, total),
        out_shape=jax.ShapeDtypeStruct((2 * pts, lanes), jnp.float32),
        in_specs=[smem, anywhere, vmem, vmem, anywhere, anywhere, anywhere],
        out_specs=vmem,
        scratch_shapes=[
            pltpu.VMEM((own, width), jnp.bfloat16),
            dma,
            pltpu.VMEM((3, NUM_PIECES, vocab, kp), jnp.bfloat16),
            pltpu.VMEM((NUM_PIECES, lanes, kp), jnp.bfloat16),
            pltpu.VMEM((3, vocab, lanes), jnp.float32),
            pltpu.VMEM((2 * pts, lanes), jnp.float32),
            pltpu.VMEM((n_grid, 2 * pts, lanes), jnp.float32),
            pltpu.VMEM((n_grid, 2 * pts, lanes), jnp.float32),
            pltpu.VMEM((n_fsdp, n_grid, 2 * pts, lanes), jnp.float32),
            dma((3, NUM_PIECES)),
            dma((NUM_PIECES,)),
            dma((NUM_PIECES,)),
            dma((NUM_PIECES,)),
            dma((NUM_PIECES,)),
            dma((NUM_PIECES,)),
            dma((n_grid - 1,)),
            dma((n_grid,)),
            dma((n_all - 1,)),
            dma((n_all,)),
            pltpu.SemaphoreType.REGULAR,
        ],
        compiler_params=pltpu.CompilerParams(
            collective_id=0, has_side_effects=True, vmem_limit_bytes=60 * 1024 * 1024
        ),
    )(
        coords, hidden, norm_gain.reshape(1, width), targets.reshape(n_grid, lanes),
        base_head, first_dir, second_dir,
    )
    return tuple(
        pl.pallas_call(
            split,
            out_shape=(
                jax.ShapeDtypeStruct((pts, own), jnp.float32),
                jax.ShapeDtypeStruct((pts,), jnp.float32),
            ),
            in_specs=[vmem],
            out_specs=(vmem, smem),
        )(packed)
    )


def solution(mesh):
    placed = (
        P("fsdp", None),
        P(),
        P("fsdp", None),
        P("fsdp", None),
        P("fsdp", None),
        P("grid", None),
        P(),
    )
    n_grid, n_fsdp = mesh.shape["grid"], mesh.shape["fsdp"]
    return jax.shard_map(
        functools.partial(body, n_grid, n_fsdp),
        mesh=mesh, in_specs=placed, out_specs=(P("grid", "fsdp"), P("grid")), check_vma=False,
    )
```
